16 devices in a mesh: dp: 2 (over y, z), sp: 8 (over x, core).
Axes of the slice: x: 4, y: 2, z: 1, core: 2. Of those that a mesh axis runs over, the one named last changes fastest.
The devices are a block of a 4x4x8 slice.
Arguments:
- image_tokens: bfloat16 [64, 256, 1152], P('dp', 'sp'), parts along dimension 0
- ln1_gain: float32 [2, 1152], replicated
- ln1_shift: float32 [2, 1152], replicated
- w_qkv: bfloat16 [2, 1152, 3, 16, 72], replicated
- b_qkv: float32 [2, 3, 16, 72], replicated
- w_out: bfloat16 [2, 16, 72, 1152], replicated
- b_out: float32 [2, 1152], replicated
- ln2_gain: float32 [2, 1152], replicated
- ln2_shift: float32 [2, 1152], replicated
- w_up: bfloat16 [2, 1152, 4304], replicated
- b_up: float32 [2, 4304], replicated
- w_down: bfloat16 [2, 4304, 1152], replicated
- b_down: float32 [2, 1152], replicated
Outputs:
- output: bfloat16 [64, 256, 1152], P('dp', 'sp'), parts along dimension 0
There are 2 independent parts. The reference program is written for one: setup_inputs(seed, part) draws one part's arguments, and reference() takes and returns one part's arrays. A program takes and returns all parts, laid end to end along the dimension named above; an argument that names none is the same for every part.
All inputs are finite; a program needn't handle non-finite values.
Results may differ from the reference program's by a relative error of at most 0.014371.
Values are sent between devices in bfloat16 or wider.
A program may use at most 768 MiB of HBM per device.

```python
import jax
import jax.numpy as jnp
from jax import lax

IMAGES = 32
SEQ_LEN = 256
WIDTH = 1152
HEADS = 16
HEAD_DIM = 72
MLP_DIM = 4304
LAYERS = 2
LN_EPS = 1e-6


def layer_norm(tokens, ln_gain, ln_shift):
    values = tokens.astype(jnp.float32)
    mean_val = jnp.mean(values, axis=-1, keepdims=True)
    centred = values - mean_val
    var_val = jnp.mean(centred * centred, axis=-1, keepdims=True)
    return (centred * lax.rsqrt(var_val + LN_EPS) * ln_gain + ln_shift).astype(jnp.bfloat16)


def one_head(head_inputs):
    q_head, k_head, v_head = head_inputs
    score_scale = q_head.shape[-1] ** -0.5
    scores = jnp.einsum('bqe,bke->bqk', q_head.astype(jnp.float32), k_head.astype(jnp.float32)) * score_scale
    row_peak = jnp.max(scores, axis=-1, keepdims=True)
    prob_vals = jnp.exp(scores - row_peak)
    row_total = jnp.sum(prob_vals, axis=-1, keepdims=True)
    mixed_vals = jnp.einsum('bqk,bke->bqe', prob_vals.astype(jnp.bfloat16).astype(jnp.float32), v_head.astype(jnp.float32))
    return (mixed_vals / row_total).astype(jnp.bfloat16)


def encoder_layer(hidden, layer_params):
    (ln1_gain, ln1_shift, w_qkv, b_qkv, w_out, b_out, ln2_gain, ln2_shift, w_up, b_up, w_down, b_down) = layer_params
    normed = layer_norm(hidden, ln1_gain, ln1_shift)
    qkv_all = jnp.einsum('bsd,dthe->bsthe', normed.astype(jnp.float32), w_qkv.astype(jnp.float32)) + b_qkv
    per_head = jnp.moveaxis(qkv_all.astype(jnp.bfloat16), 3, 0)
    heads_out = lax.map(one_head, (per_head[:, :, :, 0], per_head[:, :, :, 1], per_head[:, :, :, 2]))
    attn_proj = jnp.einsum('hbse,hed->bsd', heads_out.astype(jnp.float32), w_out.astype(jnp.float32)) + b_out
    mid_state = (hidden.astype(jnp.float32) + attn_proj).astype(jnp.bfloat16)
    normed_two = layer_norm(mid_state, ln2_gain, ln2_shift)
    up_proj = jnp.einsum('bsd,df->bsf', normed_two.astype(jnp.float32), w_up.astype(jnp.float32)) + b_up
    active = jax.nn.gelu(up_proj, approximate=True).astype(jnp.bfloat16)
    down_proj = jnp.einsum('bsf,fd->bsd', active.astype(jnp.float32), w_down.astype(jnp.float32)) + b_down
    return (mid_state.astype(jnp.float32) + down_proj).astype(jnp.bfloat16)


def setup_inputs(seed: int = 0, part: int = 0) -> dict:
    part_key = jax.random.fold_in(jax.random.key(seed), part)
    key_pattern, key_noise = jax.random.split(part_key, 2)
    period = SEQ_LEN // 8
    half_width = WIDTH // 2
    pattern = jax.random.normal(key_pattern, (IMAGES, period, half_width), jnp.float32)
    repeated = jnp.tile(pattern, (1, SEQ_LEN // period, 1))
    noise_part = jax.random.normal(key_noise, (IMAGES, SEQ_LEN, WIDTH - half_width), jnp.float32)
    image_tokens = jnp.concatenate([repeated, noise_part], axis=-1).astype(jnp.bfloat16)
    key_set = jax.random.split(jax.random.key(seed + 1), 14)
    row_scale = jnp.where(jnp.arange(WIDTH) < half_width, 1.0, 0.2)[:, None, None]
    head_shape = (LAYERS, WIDTH, HEADS, HEAD_DIM)
    w_query = 2.0 * WIDTH ** -0.5 * row_scale * jax.random.normal(key_set[0], head_shape, jnp.float32)
    w_key = w_query + 0.1 * WIDTH ** -0.5 * jax.random.normal(key_set[1], head_shape, jnp.float32)
    w_value = WIDTH ** -0.5 * jax.random.normal(key_set[2], head_shape, jnp.float32)
    w_qkv = jnp.stack([w_query, w_key, w_value], axis=2).astype(jnp.bfloat16)
    b_qkv = 0.3 * jax.random.normal(key_set[3], (LAYERS, 3, HEADS, HEAD_DIM), jnp.float32)
    w_out = (1.5 * WIDTH ** -0.5 * jax.random.normal(key_set[4], (LAYERS, HEADS, HEAD_DIM, WIDTH), jnp.float32)).astype(jnp.bfloat16)
    b_out = 0.3 * jax.random.normal(key_set[5], (LAYERS, WIDTH), jnp.float32)
    ln1_gain = 1.0 + 0.2 * jax.random.normal(key_set[6], (LAYERS, WIDTH), jnp.float32)
    ln1_shift = 0.3 * jax.random.normal(key_set[7], (LAYERS, WIDTH), jnp.float32)
    ln2_gain = 1.0 + 0.2 * jax.random.normal(key_set[8], (LAYERS, WIDTH), jnp.float32)
    ln2_shift = 0.3 * jax.random.normal(key_set[9], (LAYERS, WIDTH), jnp.float32)
    w_up = (WIDTH ** -0.5 * jax.random.normal(key_set[10], (LAYERS, WIDTH, MLP_DIM), jnp.float32)).astype(jnp.bfloat16)
    b_up = 0.3 * jax.random.normal(key_set[11], (LAYERS, MLP_DIM), jnp.float32)
    w_down = (0.5 * MLP_DIM ** -0.5 * jax.random.normal(key_set[12], (LAYERS, MLP_DIM, WIDTH), jnp.float32)).astype(jnp.bfloat16)
    b_down = 0.3 * jax.random.normal(key_set[13], (LAYERS, WIDTH), jnp.float32)
    return {'image_tokens': image_tokens, 'ln1_gain': ln1_gain, 'ln1_shift': ln1_shift, 'w_qkv': w_qkv, 'b_qkv': b_qkv, 'w_out': w_out, 'b_out': b_out, 'ln2_gain': ln2_gain, 'ln2_shift': ln2_shift, 'w_up': w_up, 'b_up': b_up, 'w_down': w_down, 'b_down': b_down}


def reference(image_tokens, ln1_gain, ln1_shift, w_qkv, b_qkv, w_out, b_out, ln2_gain, ln2_shift, w_up, b_up, w_down, b_down):
    stacked = (ln1_gain, ln1_shift, w_qkv, b_qkv, w_out, b_out, ln2_gain, ln2_shift, w_up, b_up, w_down, b_down)

    def layer_body(hidden, layer_params):
        return encoder_layer(hidden, layer_params), None

    return lax.scan(layer_body, image_tokens, stacked)[0]
```

```python
import jax
import jax.numpy as jnp
from jax import lax
from jax.sharding import PartitionSpec as P

LN_EPS = 1e-6


def layer_norm(tokens, ln_gain, ln_shift):
    values = tokens.astype(jnp.float32)
    mean_val = jnp.mean(values, axis=-1, keepdims=True)
    centred = values - mean_val
    var_val = jnp.mean(centred * centred, axis=-1, keepdims=True)
    return (centred * lax.rsqrt(var_val + LN_EPS) * ln_gain + ln_shift).astype(jnp.bfloat16)


def attend(q_part, k_part, v_part):
    score_scale = q_part.shape[-1] ** -0.5
    scores = jnp.einsum('bqhe,bkhe->bhqk', q_part, k_part, preferred_element_type=jnp.float32) * score_scale
    row_peak = jnp.max(scores, axis=-1, keepdims=True)
    prob_vals = jnp.exp(scores - row_peak)
    row_total = jnp.sum(prob_vals, axis=-1, keepdims=True)
    mixed_vals = jnp.einsum('bhqk,bkhe->bhqe', prob_vals.astype(jnp.bfloat16), v_part, preferred_element_type=jnp.float32)
    return (mixed_vals / row_total).astype(jnp.bfloat16)


def mlp_block(mid_state, ln2_gain, ln2_shift, w_up, b_up, w_down, b_down):
    normed = layer_norm(mid_state, ln2_gain, ln2_shift)
    up_proj = jnp.einsum('bsd,df->bsf', normed, w_up, preferred_element_type=jnp.float32) + b_up
    active = jax.nn.gelu(up_proj, approximate=True).astype(jnp.bfloat16)
    down_proj = jnp.einsum('bsf,fd->bsd', active, w_down, preferred_element_type=jnp.float32) + b_down
    return (mid_state.astype(jnp.float32) + down_proj).astype(jnp.bfloat16)


def solution(mesh):
    token_spec = P('dp', 'sp', None)

    def device_step(image_tokens, ln1_gain, ln1_shift, w_qkv, b_qkv, w_out, b_out, ln2_gain, ln2_shift, w_up, b_up, w_down, b_down):
        hidden = lax.all_to_all(image_tokens, 'sp', 0, 1, tiled=True)
        for layer_idx in range(w_qkv.shape[0]):
            normed = layer_norm(hidden, ln1_gain[layer_idx], ln1_shift[layer_idx])
            qkv = (jnp.einsum('bsd,dthe->bsthe', normed, w_qkv[layer_idx], preferred_element_type=jnp.float32) + b_qkv[layer_idx]).astype(jnp.bfloat16)
            attn = attend(qkv[:, :, 0], qkv[:, :, 1], qkv[:, :, 2])
            attn_proj = jnp.einsum('bhse,hed->bsd', attn, w_out[layer_idx], preferred_element_type=jnp.float32) + b_out[layer_idx]
            mid_state = (hidden.astype(jnp.float32) + attn_proj).astype(jnp.bfloat16)
            hidden = mlp_block(mid_state, ln2_gain[layer_idx], ln2_shift[layer_idx], w_up[layer_idx], b_up[layer_idx], w_down[layer_idx], b_down[layer_idx])
        return lax.all_to_all(hidden, 'sp', 1, 0, tiled=True)

    return jax.shard_map(device_step, mesh=mesh, in_specs=(token_spec,) + (P(),) * 12, out_specs=token_spec, check_vma=False)
```

```python
import functools
import math

import jax
import jax.numpy as jnp
from jax import lax
from jax.experimental import pallas as pl
from jax.experimental.pallas import tpu as pltpu
from jax.sharding import PartitionSpec as P

LN_EPS = 1e-6
F32 = jnp.float32
BF16 = jnp.bfloat16
LANES = 128


def dot(a, b, ca, cb):
    return lax.dot_general(a, b, (((ca,), (cb,)), ((), ())), preferred_element_type=F32)


def blocks(total, size):
    return [(s, min(size, total - s)) for s in range(0, total, size)]


def row_norm(values, gain, shift):
    mean_val = jnp.mean(values, axis=-1, keepdims=True)
    centred = values - mean_val
    var_val = jnp.mean(centred * centred, axis=-1, keepdims=True)
    return (centred * lax.rsqrt(var_val + LN_EPS) * gain + shift).astype(BF16)


def encoder_kernel(axes, heads, head_dim, x_ref, wq_hbm, wo_hbm, wu_hbm, wd_hbm, bq_ref, bu_ref,
                   g1_ref, s1_ref, bo_ref, g2_ref, s2_ref, bd_ref, out_ref,
                   hid, wq, wo, wu, wd, bq_col, bu_col, normed, qkv, mixed, active,
                   w_sem, in_send, in_recv, in_local, out_send, out_recv, out_local):
    dp_axis, sp_axis = axes
    slots, tokens, width = hid.shape
    layers, mlp = bu_ref.shape
    peers = lax.axis_size(sp_axis)
    share = tokens // peers
    me = lax.axis_index(sp_axis)
    dp_me = lax.axis_index(dp_axis)
    score_scale = head_dim ** -0.5 * math.log2(math.e)

    def peer(offset):
        return lax.rem(me + offset, peers)

    def target(offset):
        return (dp_me, peer(offset))

    weights = ((wq_hbm, wq), (wo_hbm, wo), (wu_hbm, wu), (wd_hbm, wd))

    def weight_copy(which, layer):
        src, dst = weights[which]
        return pltpu.make_async_copy(src.at[layer], dst, w_sem.at[which])

    for which in range(4):
        weight_copy(which, 0).start()

    barrier = pltpu.get_barrier_semaphore()
    for offset in range(1, peers):
        pl.semaphore_signal(barrier, inc=1, device_id=target(offset), device_id_type=pl.DeviceIdType.MESH)
    pl.semaphore_wait(barrier, peers - 1)

    def in_copy(slot, offset):
        return pltpu.make_async_remote_copy(
            src_ref=x_ref.at[peer(offset) * slots + slot],
            dst_ref=hid.at[slot, pl.ds(me * share, share), :],
            send_sem=in_send.at[slot, offset], recv_sem=in_recv.at[slot, offset],
            device_id=target(offset), device_id_type=pl.DeviceIdType.MESH)

    def in_own(slot):
        return pltpu.make_async_copy(x_ref.at[me * slots + slot], hid.at[slot, pl.ds(me * share, share), :], in_local.at[slot])

    def out_copy(slot, offset):
        return pltpu.make_async_remote_copy(
            src_ref=hid.at[slot, pl.ds(peer(offset) * share, share), :],
            dst_ref=out_ref.at[me * slots + slot],
            send_sem=out_send.at[slot, offset], recv_sem=out_recv.at[slot, offset],
            device_id=target(offset), device_id_type=pl.DeviceIdType.MESH)

    def out_own(slot):
        return pltpu.make_async_copy(hid.at[slot, pl.ds(me * share, share), :], out_ref.at[me * slots + slot], out_local.at[slot])

    for slot in range(slots):
        for offset in range(1, peers):
            in_copy(slot, offset).start()
        in_own(slot).start()

    def columns(row):
        return jnp.transpose(jnp.broadcast_to(row, (LANES, row.shape[-1])))

    for layer in range(layers):
        @pl.loop(0, 3 * heads)
        def _(j):
            row = bq_ref[layer, pl.ds(j, 1), :]
            bq_col[layer, pl.ds(pl.multiple_of(j * head_dim, 8), head_dim), :] = columns(row)
        for start, size in blocks(mlp, LANES):
            bu_col[layer, start:start + size, :] = columns(bu_ref[layer:layer + 1, start:start + size])

    def wide(col):
        return jnp.concatenate([col] * (tokens // LANES), axis=1)

    def pick(ref, layer, cols):
        value = ref[0:1, cols]
        for other in range(1, layers):
            value = jnp.where(layer == other, ref[other:other + 1, cols], value)
        return value

    def norm_to(layer, slot, gain_ref, shift_ref):
        gain, shift = pick(gain_ref, layer, slice(None)), pick(shift_ref, layer, slice(None))
        for start, size in blocks(tokens, 32):
            rows = slice(start, start + size)
            normed[rows, :] = row_norm(hid[slot, rows, :].astype(F32), gain, shift)

    def step(index, carry):
        layer = index // slots
        slot = lax.rem(index, slots)

        @pl.when(layer == 0)
        def _():
            for offset in range(1, peers):
                in_copy(slot, offset).wait_recv()
            in_own(slot).wait()

        def await_weight(which):
            @pl.when(slot == 0)
            def _():
                weight_copy(which, layer).wait()

        def next_weight(which):
            @pl.when(jnp.logical_and(slot == slots - 1, layer < layers - 1))
            def _():
                weight_copy(which, layer + 1).start()

        norm_to(layer, slot, g1_ref, s1_ref)
        await_weight(0)
        for start, size in blocks(3 * width, 512):
            rows = slice(start, start + size)
            part = dot(wq[rows, :], normed[...], 1, 1)
            qkv[rows, :] = (part + wide(bq_col[layer, rows, :])).astype(BF16)
        next_weight(0)

        for head in range(heads):
            rows = slice(head * head_dim, (head + 1) * head_dim)
            q_part = qkv[rows, :]
            k_part = qkv[width + head * head_dim:width + (head + 1) * head_dim, :]
            v_part = qkv[2 * width + head * head_dim:2 * width + (head + 1) * head_dim, :]
            scores = dot(k_part, q_part, 0, 0)
            peak = jnp.max(scores, axis=0, keepdims=True)
            prob = jnp.exp2((scores - peak) * score_scale)
            total = jnp.sum(prob, axis=0, keepdims=True)
            mix = dot(v_part, prob.astype(BF16), 1, 0)
            mixed[rows, :] = (mix * (1.0 / total)).astype(BF16)

        await_weight(1)
        for start, size in blocks(width, 256):
            cols = slice(start, start + size)
            part = dot(mixed[...], wo[:, cols], 0, 0) + pick(bo_ref, layer, cols)
            hid[slot, :, cols] = (hid[slot, :, cols].astype(F32) + part).astype(BF16)
        next_weight(1)

        norm_to(layer, slot, g2_ref, s2_ref)
        await_weight(2)
        for start, size in blocks(mlp, 512):
            rows = slice(start, start + size)
            part = dot(wu[rows, :], normed[...], 1, 1) + wide(bu_col[layer, rows, :])
            active[rows, :] = jax.nn.gelu(part, approximate=True).astype(BF16)
        next_weight(2)

        await_weight(3)
        for start, size in blocks(width, 256):
            cols = slice(start, start + size)
            part = dot(active[...], wd[:, cols], 0, 0) + pick(bd_ref, layer, cols)
            hid[slot, :, cols] = (hid[slot, :, cols].astype(F32) + part).astype(BF16)
        next_weight(3)

        @pl.when(layer == layers - 1)
        def _():
            for offset in range(1, peers):
                out_copy(slot, offset).start()
            out_own(slot).start()
        return carry

    lax.fori_loop(0, layers * slots, step, 0)

    for slot in range(slots):
        for offset in range(1, peers):
            in_copy(slot, offset).wait_send()
            out_copy(slot, offset).wait()
        out_own(slot).wait()


def solution(mesh):
    token_spec = P('dp', 'sp', None)
    peers = mesh.shape['sp']

    def device_step(image_tokens, ln1_gain, ln1_shift, w_qkv, b_qkv, w_out, b_out, ln2_gain, ln2_shift, w_up, b_up, w_down, b_down):
        layers, width, _, heads, head_dim = w_qkv.shape
        mlp = w_up.shape[-1]
        images, share, _ = image_tokens.shape
        slots, tokens = images // peers, share * peers
        wq_t = jnp.transpose(w_qkv, (0, 2, 3, 4, 1)).reshape(layers, 3 * width, width)
        wu_t = jnp.transpose(w_up, (0, 2, 1))
        wo = w_out.reshape(layers, width, width)
        bq = b_qkv.reshape(layers, 3 * heads, head_dim)
        hbm = pl.BlockSpec(memory_space=pl.ANY)
        vmem = pl.BlockSpec(memory_space=pltpu.VMEM)
        dma = pltpu.SemaphoreType.DMA
        return pl.pallas_call(
            functools.partial(encoder_kernel, ('dp', 'sp'), heads, head_dim),
            out_shape=jax.ShapeDtypeStruct(image_tokens.shape, image_tokens.dtype),
            in_specs=[hbm] * 5 + [vmem] * 8,
            out_specs=hbm,
            scratch_shapes=[
                pltpu.VMEM((slots, tokens, width), BF16),
                pltpu.VMEM((3 * width, width), BF16),
                pltpu.VMEM((width, width), BF16),
                pltpu.VMEM((mlp, width), BF16),
                pltpu.VMEM((mlp, width), BF16),
                pltpu.VMEM((layers, 3 * width, LANES), F32),
                pltpu.VMEM((layers, mlp, LANES), F32),
                pltpu.VMEM((tokens, width), BF16),
                pltpu.VMEM((3 * width, tokens), BF16),
                pltpu.VMEM((width, tokens), BF16),
                pltpu.VMEM((mlp, tokens), BF16),
                dma((4,)), dma((slots, peers)), dma((slots, peers)), dma((slots,)),
                dma((slots, peers)), dma((slots, peers)), dma((slots,)),
            ],
            compiler_params=pltpu.CompilerParams(collective_id=0, has_side_effects=True, vmem_limit_bytes=64000 * 1024),
        )(image_tokens, wq_t, wo, wu_t, w_down, bq, b_up, ln1_gain, ln1_shift, b_out, ln2_gain, ln2_shift, b_down)

    return jax.shard_map(device_step, mesh=mesh, in_specs=(token_spec,) + (P(),) * 12, out_specs=token_spec, check_vma=False)
```

```python
import functools
import math

import jax
import jax.numpy as jnp
from jax import lax
from jax.experimental import pallas as pl
from jax.experimental.pallas import tpu as pltpu
from jax.sharding import PartitionSpec as P

LN_EPS = 1e-6
F32 = jnp.float32
BF16 = jnp.bfloat16
LANES = 128
LAG = 2
DEPTH = 2 * LAG + 1
HEAD_GROUP = 4
OUT_ROWS = 128
UP_ROWS = 256
SPLIT = 512


def dot(a, b, ca, cb):
    return lax.dot_general(a, b, (((ca,), (cb,)), ((), ())), preferred_element_type=F32)


def blocks(total, size):
    return [(s, min(size, total - s)) for s in range(0, total, size)]


def row_norm(values, gain, shift):
    mean_val = jnp.mean(values, axis=-1, keepdims=True)
    centred = values - mean_val
    var_val = jnp.mean(centred * centred, axis=-1, keepdims=True)
    return (centred * lax.rsqrt(var_val + LN_EPS) * gain + shift).astype(BF16)


def encoder_kernel(axes, heads, head_dim, x_hbm, wq_hbm, wo_hbm, wu_hbm, wd_hbm, bq_hbm, bu_hbm,
                   g1_hbm, s1_hbm, bo_hbm, g2_hbm, s2_hbm, bd_hbm, out_ref,
                   hid, stage, wq, wo, wu, wd, bq_ref, bu_ref, g1_ref, s1_ref, bo_ref, g2_ref, s2_ref, bd_ref,
                   bq_col, bu_col, normed, mid, qkv, mixed, active, scores, probs,
                   w_sem, p_sem, x_sem, in_send, in_recv, in_local, out_send, out_recv, out_local):
    dp_axis, sp_axis = axes
    slots, tokens, width = hid.shape
    layers, mlp = bu_ref.shape
    peers = lax.axis_size(sp_axis)
    share = tokens // peers
    me = lax.axis_index(sp_axis)
    dp_me = lax.axis_index(dp_axis)
    score_scale = head_dim ** -0.5 * math.log2(math.e)

    def peer(offset):
        return lax.rem(me + offset, peers)

    def target(offset):
        return (dp_me, peer(offset))

    weights = ((wq_hbm, wq), (wo_hbm, wo), (wu_hbm, wu), (wd_hbm, wd))
    smalls = ((bq_hbm, bq_ref), (bu_hbm, bu_ref), (g1_hbm, g1_ref), (s1_hbm, s1_ref),
              (bo_hbm, bo_ref), (g2_hbm, g2_ref), (s2_hbm, s2_ref), (bd_hbm, bd_ref))

    def weight_copy(which, layer):
        src, dst = weights[which]
        return pltpu.make_async_copy(src.at[layer], dst, w_sem.at[which])

    def small_copy(which):
        src, dst = smalls[which]
        return pltpu.make_async_copy(src, dst, p_sem.at[which])

    def in_copy(slot, offset):
        return pltpu.make_async_remote_copy(
            src_ref=stage.at[peer(offset) * slots + slot],
            dst_ref=hid.at[slot, pl.ds(me * share, share), :],
            send_sem=in_send.at[slot, offset], recv_sem=in_recv.at[slot, offset],
            device_id=target(offset), device_id_type=pl.DeviceIdType.MESH)

    def in_own(slot):
        return pltpu.make_async_copy(x_hbm.at[me * slots + slot], hid.at[slot, pl.ds(me * share, share), :], in_local.at[slot])

    def out_copy(slot, offset, cols=slice(None)):
        return pltpu.make_async_remote_copy(
            src_ref=hid.at[slot, pl.ds(peer(offset) * share, share), cols],
            dst_ref=out_ref.at[me * slots + slot, :, cols],
            send_sem=out_send.at[slot, offset], recv_sem=out_recv.at[slot, offset],
            device_id=target(offset), device_id_type=pl.DeviceIdType.MESH)

    def out_own(slot):
        return pltpu.make_async_copy(hid.at[slot, pl.ds(me * share, share), :], out_ref.at[me * slots + slot], out_local.at[slot])

    for which in range(len(smalls)):
        small_copy(which).start()
    fetch = pltpu.make_async_copy(x_hbm, stage, x_sem.at[0])
    fetch.start()
    weight_copy(0, 0).start()
    for slot in range(slots):
        in_own(slot).start()
    barrier = pltpu.get_barrier_semaphore()
    for offset in range(1, peers):
        pl.semaphore_signal(barrier, inc=1, device_id=target(offset), device_id_type=pl.DeviceIdType.MESH)

    def columns(row):
        return jnp.transpose(jnp.broadcast_to(row, (LANES, row.shape[-1])))

    def build_columns(layer):
        for start in range(3 * heads):
            rows = slice(start * head_dim, (start + 1) * head_dim)
            bq_col[layer, rows, :] = columns(bq_ref[layer, start:start + 1, :])
        for start, size in blocks(mlp, LANES):
            bu_col[layer, start:start + size, :] = columns(bu_ref[layer:layer + 1, start:start + size])

    for which in range(len(smalls)):
        small_copy(which).wait()
    build_columns(0)
    fetch.wait()
    pl.semaphore_wait(barrier, peers - 1)
    for slot in range(slots):
        for offset in range(1, peers):
            in_copy(slot, offset).start()
    weight_copy(0, 0).wait()
    for which in range(1, 4):
        weight_copy(which, 0).start()
    for layer in range(1, layers):
        build_columns(layer)
    for which in range(1, 4):
        weight_copy(which, 0).wait()

    def wide(col):
        return jnp.concatenate([col] * (tokens // LANES), axis=1)

    def pick(ref, layer, cols):
        value = ref[0:1, cols]
        for other in range(1, layers):
            value = jnp.where(layer == other, ref[other:other + 1, cols], value)
        return value

    def norm_rows(layer, source, gain_ref, shift_ref, first, count):
        gain, shift = pick(gain_ref, layer, slice(None)), pick(shift_ref, layer, slice(None))
        for start, size in blocks(count, 32):
            rows = slice(first + start, first + start + size)
            normed[rows, :] = row_norm(source[rows, :].astype(F32), gain, shift)

    def body(index, layer, slot, edge):
        loads = jnp.logical_and(slot == slots - 1, layer < layers - 1)
        waits = jnp.logical_and(slot == 0, layer > 0)
        final = index == layers * slots - 1

        def manage(awaited, fetched):
            if edge:
                @pl.when(waits)
                def _():
                    for which in awaited:
                        weight_copy(which, layer).wait()

                @pl.when(loads)
                def _():
                    for which in fetched:
                        weight_copy(which, layer + 1).start()

        norm_rows(layer, hid.at[slot], g1_ref, s1_ref, 0, tokens)
        totals = {}

        def project(start, size):
            rows = slice(start, start + size)
            part = dot(wq[rows, :], normed[...], 1, 1)
            qkv[rows, :] = (part + wide(bq_col[layer, rows, :])).astype(BF16)

        def score(head):
            q_part = qkv[head * head_dim:(head + 1) * head_dim, :]
            k_part = qkv[width + head * head_dim:width + (head + 1) * head_dim, :]
            scores[head % DEPTH] = dot(k_part, q_part, 0, 0)

        def soften(head):
            values = scores[head % DEPTH]
            prob = jnp.exp2((values - jnp.max(values, axis=0, keepdims=True)) * score_scale)
            totals[head] = jnp.sum(prob, axis=0, keepdims=True)
            probs[head % DEPTH] = prob.astype(BF16)

        def mix(head):
            v_part = qkv[2 * width + head * head_dim:2 * width + (head + 1) * head_dim, :]
            part = dot(v_part, probs[head % DEPTH], 1, 0)
            mixed[head * head_dim:(head + 1) * head_dim, :] = (part * (1.0 / totals[head])).astype(BF16)

        chunk = HEAD_GROUP * head_dim
        todo = [(third * width + first, size) for first, size in blocks(width, chunk) for third in range(3)]
        for start, size in todo[:3]:
            project(start, size)
        todo = todo[3:]
        for turn in range(heads + 2 * LAG):
            if todo and turn % HEAD_GROUP < 3:
                project(*todo.pop(0))
            if turn < heads:
                score(turn)
            if LAG <= turn < heads + LAG:
                soften(turn - LAG)
            if turn >= 2 * LAG:
                mix(turn - 2 * LAG)
        manage((1, 2), (0,))

        for first, count in blocks(tokens, OUT_ROWS):
            picked = slice(first, first + count)
            for start, size in blocks(width, 256):
                cols = slice(start, start + size)
                part = dot(mixed[:, picked], wo[:, cols], 0, 0) + pick(bo_ref, layer, cols)
                mid[picked, cols] = (hid[slot, picked, cols].astype(F32) + part).astype(BF16)
            norm_rows(layer, mid, g2_ref, s2_ref, first, count)

        for start, size in blocks(mlp, UP_ROWS):
            rows = slice(start, start + size)
            part = dot(wu[rows, :], normed[...], 1, 1) + wide(bu_col[layer, rows, :])
            active[rows, :] = jax.nn.gelu(part, approximate=True).astype(BF16)
        manage((3,), (1, 2))

        for start, size in blocks(width, 256):
            cols = slice(start, start + size)
            part = dot(active[...], wd[:, cols], 0, 0) + pick(bd_ref, layer, cols)
            hid[slot, :, cols] = (mid[:, cols].astype(F32) + part).astype(BF16)
            if edge and start == SPLIT - 256:
                @pl.when(final)
                def _():
                    for offset in range(1, peers):
                        out_copy(slot, offset, slice(0, SPLIT)).start()

    def step(index, carry):
        layer = index // slots
        slot = lax.rem(index, slots)
        final = index == layers * slots - 1
        edge = jnp.logical_or(jnp.logical_or(final, jnp.logical_and(slot == slots - 1, layer < layers - 1)),
                              jnp.logical_and(slot == 0, layer > 0))

        @pl.when(layer == 0)
        def _():
            for offset in range(1, peers):
                in_copy(slot, offset).wait_recv()
            in_own(slot).wait()

        @pl.when(jnp.logical_and(slot == 0, layer > 0))
        def _():
            weight_copy(0, layer).wait()

        @pl.when(edge)
        def _():
            body(index, layer, slot, True)

        @pl.when(jnp.logical_not(edge))
        def _():
            body(index, layer, slot, False)

        @pl.when(jnp.logical_and(slot == slots - 1, layer < layers - 1))
        def _():
            weight_copy(3, layer + 1).start()

        @pl.when(layer == layers - 1)
        def _():
            @pl.when(final)
            def _():
                for offset in range(1, peers):
                    out_copy(slot, offset, slice(SPLIT, width)).start()

            @pl.when(jnp.logical_not(final))
            def _():
                for offset in range(1, peers):
                    out_copy(slot, offset).start()
            out_own(slot).start()
        return carry

    lax.fori_loop(0, layers * slots, step, 0)

    for slot in range(slots):
        for offset in range(1, peers):
            in_copy(slot, offset).wait_send()
            out_copy(slot, offset).wait()
        out_own(slot).wait()


def solution(mesh):
    token_spec = P('dp', 'sp', None)
    peers = mesh.shape['sp']

    def device_step(image_tokens, ln1_gain, ln1_shift, w_qkv, b_qkv, w_out, b_out, ln2_gain, ln2_shift, w_up, b_up, w_down, b_down):
        layers, width, _, heads, head_dim = w_qkv.shape
        mlp = w_up.shape[-1]
        images, share, _ = image_tokens.shape
        slots, tokens = images // peers, share * peers
        wq_t = jnp.transpose(w_qkv, (0, 2, 3, 4, 1)).reshape(layers, 3 * width, width)
        wu_t = jnp.transpose(w_up, (0, 2, 1))
        wo = w_out.reshape(layers, width, width)
        bq = b_qkv.reshape(layers, 3 * heads, head_dim)
        hbm = pl.BlockSpec(memory_space=pl.ANY)
        vmem = pl.BlockSpec(memory_space=pltpu.VMEM)
        dma = pltpu.SemaphoreType.DMA
        return pl.pallas_call(
            functools.partial(encoder_kernel, ('dp', 'sp'), heads, head_dim),
            out_shape=pltpu.VMEM(image_tokens.shape, image_tokens.dtype),
            in_specs=[hbm] * 13,
            out_specs=vmem,
            scratch_shapes=[
                pltpu.VMEM((slots, tokens, width), BF16),
                pltpu.VMEM(image_tokens.shape, BF16),
                pltpu.VMEM((3 * width, width), BF16),
                pltpu.VMEM((width, width), BF16),
                pltpu.VMEM((mlp, width), BF16),
                pltpu.VMEM((mlp, width), BF16),
                pltpu.VMEM(bq.shape, F32),
                pltpu.VMEM((layers, mlp), F32),
                *[pltpu.VMEM((layers, width), F32)] * 6,
                pltpu.VMEM((layers, 3 * width, LANES), F32),
                pltpu.VMEM((layers, mlp, LANES), F32),
                pltpu.VMEM((tokens, width), BF16),
                pltpu.VMEM((tokens, width), BF16),
                pltpu.VMEM((3 * width, tokens), BF16),
                pltpu.VMEM((width, tokens), BF16),
                pltpu.VMEM((mlp, tokens), BF16),
                pltpu.VMEM((DEPTH, tokens, tokens), F32),
                pltpu.VMEM((DEPTH, tokens, tokens), BF16),
                dma((4,)), dma((8,)), dma((1,)), dma((slots, peers)), dma((slots, peers)), dma((slots,)),
                dma((slots, peers)), dma((slots, peers)), dma((slots,)),
            ],
            compiler_params=pltpu.CompilerParams(collective_id=0, has_side_effects=True, vmem_limit_bytes=60000 * 1024),
        )(image_tokens, wq_t, wo, wu_t, w_down, bq, b_up, ln1_gain, ln1_shift, b_out, ln2_gain, ln2_shift, b_down)

    return jax.shard_map(device_step, mesh=mesh, in_specs=(token_spec,) + (P(),) * 12, out_specs=token_spec, check_vma=False)
```

```python
import functools
import math

import jax
import jax.numpy as jnp
from jax import lax
from jax.experimental import pallas as pl
from jax.experimental.pallas import tpu as pltpu
from jax.sharding import PartitionSpec as P

LN_EPS = 1e-6
F32 = jnp.float32
BF16 = jnp.bfloat16
LANES = 128
LAG = 2
DEPTH = 2 * LAG + 1
HEAD_GROUP = 4
NORM_ROWS = 32
UP_ROWS = 256
SPLIT = 512


def dot(a, b, ca, cb):
    return lax.dot_general(a, b, (((ca,), (cb,)), ((), ())), preferred_element_type=F32)


def blocks(total, size):
    return [(s, min(size, total - s)) for s in range(0, total, size)]


def row_norm(values, gain, shift):
    mean_val = jnp.mean(values, axis=-1, keepdims=True)
    centred = values - mean_val
    var_val = jnp.mean(centred * centred, axis=-1, keepdims=True)
    return (centred * lax.rsqrt(var_val + LN_EPS) * gain + shift).astype(BF16)


def encoder_kernel(axes, heads, head_dim, x_hbm, wq_hbm, wo_hbm, wu_hbm, wd_hbm, bq_hbm, bu_hbm,
                   g1_hbm, s1_hbm, bo_hbm, g2_hbm, s2_hbm, bd_hbm, out_ref,
                   hid, stage, wq, wo, wu, wd, bq_ref, bu_ref, g1_ref, s1_ref, bo_ref, g2_ref, s2_ref, bd_ref,
                   bq_col, bu_col, normed, normed_mid, mid, mid_next, qkv, mixed, active, scores, probs,
                   w_sem, p_sem, x_sem, in_send, in_recv, in_local, out_send, out_recv, out_local):
    dp_axis, sp_axis = axes
    slots, tokens, width = hid.shape
    layers, mlp = bu_ref.shape
    peers = lax.axis_size(sp_axis)
    share = tokens // peers
    me = lax.axis_index(sp_axis)
    dp_me = lax.axis_index(dp_axis)
    score_scale = head_dim ** -0.5 * math.log2(math.e)

    def peer(offset):
        return lax.rem(me + offset, peers)

    def target(offset):
        return (dp_me, peer(offset))

    weights = ((wq_hbm, wq), (wo_hbm, wo), (wu_hbm, wu), (wd_hbm, wd))
    smalls = ((bq_hbm, bq_ref), (bu_hbm, bu_ref), (g1_hbm, g1_ref), (s1_hbm, s1_ref),
              (bo_hbm, bo_ref), (g2_hbm, g2_ref), (s2_hbm, s2_ref), (bd_hbm, bd_ref))

    def weight_copy(which, layer):
        src, dst = weights[which]
        return pltpu.make_async_copy(src.at[layer], dst, w_sem.at[which])

    def small_copy(which):
        src, dst = smalls[which]
        return pltpu.make_async_copy(src, dst, p_sem.at[which])

    def in_copy(slot, offset):
        return pltpu.make_async_remote_copy(
            src_ref=stage.at[peer(offset) * slots + slot],
            dst_ref=hid.at[slot, pl.ds(me * share, share), :],
            send_sem=in_send.at[slot, offset], recv_sem=in_recv.at[slot, offset],
            device_id=target(offset), device_id_type=pl.DeviceIdType.MESH)

    def in_own(slot):
        return pltpu.make_async_copy(x_hbm.at[me * slots + slot], hid.at[slot, pl.ds(me * share, share), :], in_local.at[slot])

    def out_copy(slot, offset, cols=slice(None)):
        return pltpu.make_async_remote_copy(
            src_ref=hid.at[slot, pl.ds(peer(offset) * share, share), cols],
            dst_ref=out_ref.at[me * slots + slot, :, cols],
            send_sem=out_send.at[slot, offset], recv_sem=out_recv.at[slot, offset],
            device_id=target(offset), device_id_type=pl.DeviceIdType.MESH)

    def out_own(slot):
        return pltpu.make_async_copy(hid.at[slot, pl.ds(me * share, share), :], out_ref.at[me * slots + slot], out_local.at[slot])

    for which in range(len(smalls)):
        small_copy(which).start()
    fetch = pltpu.make_async_copy(x_hbm, stage, x_sem.at[0])
    fetch.start()
    weight_copy(0, 0).start()
    for slot in range(slots):
        in_own(slot).start()
    barrier = pltpu.get_barrier_semaphore()
    for offset in range(1, peers):
        pl.semaphore_signal(barrier, inc=1, device_id=target(offset), device_id_type=pl.DeviceIdType.MESH)

    def columns(row):
        return jnp.transpose(jnp.broadcast_to(row, (LANES, row.shape[-1])))

    def build_columns(layer):
        for start in range(3 * heads):
            rows = slice(start * head_dim, (start + 1) * head_dim)
            bq_col[layer, rows, :] = columns(bq_ref[layer, start:start + 1, :])
        for start, size in blocks(mlp, LANES):
            bu_col[layer, start:start + size, :] = columns(bu_ref[layer:layer + 1, start:start + size])

    for which in range(len(smalls)):
        small_copy(which).wait()
    build_columns(0)
    fetch.wait()
    pl.semaphore_wait(barrier, peers - 1)
    for slot in range(slots):
        for offset in range(1, peers):
            in_copy(slot, offset).start()
    weight_copy(0, 0).wait()
    for which in range(1, 4):
        weight_copy(which, 0).start()
    for layer in range(1, layers):
        build_columns(layer)

    def wide(col):
        return jnp.concatenate([col] * (tokens // LANES), axis=1)

    def pick(ref, layer, cols):
        value = ref[0:1, cols]
        for other in range(1, layers):
            value = jnp.where(layer == other, ref[other:other + 1, cols], value)
        return value

    def norm_rows(target_ref, source, gain_ref, shift_ref, layer, first):
        gain, shift = pick(gain_ref, layer, slice(None)), pick(shift_ref, layer, slice(None))
        rows = slice(first, first + NORM_ROWS)
        target_ref[rows, :] = row_norm(source[rows, :].astype(F32), gain, shift)

    norm_firsts = list(range(0, tokens, NORM_ROWS))
    column_blocks = blocks(width, 256)
    up_blocks = blocks(mlp, UP_ROWS)
    gelu_scale = math.sqrt(2.0 / math.pi)

    def up_block(layer, start, size):
        rows = slice(start, start + size)
        part = dot(wu[rows, :], normed_mid[...], 1, 1) + wide(bu_col[layer, rows, :])
        inner = part * (gelu_scale + (gelu_scale * 0.044715) * (part * part))
        active[rows, :] = (part * (0.5 + 0.5 * jnp.tanh(inner))).astype(BF16)

    def down_block(layer, slot, start, size):
        cols = slice(start, start + size)
        part = dot(active[...], wd[:, cols], 0, 0) + pick(bd_ref, layer, cols)
        hid[slot, :, cols] = (mid[:, cols].astype(F32) + part).astype(BF16)

    def first_phase(layer, slot, ups):
        def up_next():
            if ups:
                ups.pop(0)()

        for order, first in enumerate(norm_firsts):
            if order % 3 == 0:
                up_next()
            norm_rows(normed, hid.at[slot], g1_ref, s1_ref, layer, first)
        totals = {}

        def project(start, size):
            rows = slice(start, start + size)
            part = dot(wq[rows, :], normed[...], 1, 1)
            qkv[rows, :] = (part + wide(bq_col[layer, rows, :])).astype(BF16)

        def score(head):
            q_part = qkv[head * head_dim:(head + 1) * head_dim, :]
            k_part = qkv[width + head * head_dim:width + (head + 1) * head_dim, :]
            scores[head % DEPTH] = dot(k_part, q_part, 0, 0)

        def soften(head):
            values = scores[head % DEPTH]
            prob = jnp.exp2((values - jnp.max(values, axis=0, keepdims=True)) * score_scale)
            totals[head] = jnp.sum(prob, axis=0, keepdims=True)
            probs[head % DEPTH] = prob.astype(BF16)

        def mix(head):
            v_part = qkv[2 * width + head * head_dim:2 * width + (head + 1) * head_dim, :]
            part = dot(v_part, probs[head % DEPTH], 1, 0)
            mixed[head * head_dim:(head + 1) * head_dim, :] = (part * (1.0 / totals[head])).astype(BF16)

        chunk = HEAD_GROUP * head_dim
        todo = [(third * width + first, size) for first, size in blocks(width, chunk) for third in range(3)]
        for start, size in todo[:3]:
            project(start, size)
        todo = todo[3:]
        for turn in range(heads + 2 * LAG):
            if todo and turn % HEAD_GROUP < 3:
                project(*todo.pop(0))
            if turn < heads:
                score(turn)
            if LAG <= turn < heads + LAG:
                soften(turn - LAG)
            if turn >= 2 * LAG:
                mix(turn - 2 * LAG)
            if turn >= 12 or turn % 2 == 1:
                up_next()
        while ups:
            up_next()

    def second_phase(layer, slot, downs):
        for start, size in column_blocks:
            cols = slice(start, start + size)
            part = dot(mixed[...], wo[:, cols], 0, 0) + pick(bo_ref, layer, cols)
            mid_next[:, cols] = (hid[slot, :, cols].astype(F32) + part).astype(BF16)
        for order, first in enumerate(norm_firsts):
            if downs and order % 2 == 0:
                downs.pop(0)()
            norm_rows(normed_mid, mid_next, g2_ref, s2_ref, layer, first)
        while downs:
            downs.pop(0)()
        mid[...] = mid_next[...]

    def ups_of(layer):
        return [functools.partial(up_block, layer, start, size) for start, size in up_blocks]

    def downs_of(layer, slot):
        return [functools.partial(down_block, layer, slot, start, size) for start, size in column_blocks]

    def arrive(slot):
        for offset in range(1, peers):
            in_copy(slot, offset).wait_recv()
        in_own(slot).wait()

    steps = layers * slots

    def step(index, carry):
        layer, slot = index // slots, lax.rem(index, slots)
        layer_mlp, slot_mlp = (index - 1) // slots, lax.rem(index - 1, slots)
        attn_last = jnp.logical_and(slot == slots - 1, layer < layers - 1)
        attn_first = jnp.logical_and(slot == 0, layer > 0)
        mlp_first = jnp.logical_and(slot_mlp == 0, layer_mlp > 0)

        @pl.when(layer == 0)
        def _():
            arrive(slot)

        @pl.when(attn_first)
        def _():
            weight_copy(0, layer).wait()

        @pl.when(mlp_first)
        def _():
            weight_copy(2, layer_mlp).wait()

        first_phase(layer, slot, ups_of(layer_mlp))

        @pl.when(attn_last)
        def _():
            weight_copy(0, layer + 1).start()

        @pl.when(attn_first)
        def _():
            weight_copy(1, layer).wait()
            weight_copy(2, layer).start()

        @pl.when(mlp_first)
        def _():
            weight_copy(3, layer_mlp).wait()

        second_phase(layer, slot, downs_of(layer_mlp, slot_mlp))

        @pl.when(attn_last)
        def _():
            weight_copy(1, layer + 1).start()

        @pl.when(attn_first)
        def _():
            weight_copy(3, layer).start()

        @pl.when(layer_mlp == layers - 1)
        def _():
            for offset in range(1, peers):
                out_copy(slot_mlp, offset).start()
            out_own(slot_mlp).start()
        return carry

    arrive(0)
    first_phase(0, 0, [])
    for which in range(1, 4):
        weight_copy(which, 0).wait()
    second_phase(0, 0, [])
    lax.fori_loop(1, steps, step, 0)

    last = slots - 1
    for block in ups_of(layers - 1):
        block()
    for (start, size), block in zip(column_blocks, downs_of(layers - 1, last)):
        block()
        if start + size == SPLIT:
            for offset in range(1, peers):
                out_copy(last, offset, slice(0, SPLIT)).start()
    for offset in range(1, peers):
        out_copy(last, offset, slice(SPLIT, width)).start()
    out_own(last).start()

    for slot in range(slots):
        for offset in range(1, peers):
            in_copy(slot, offset).wait_send()
            out_copy(slot, offset).wait()
        out_own(slot).wait()


def solution(mesh):
    token_spec = P('dp', 'sp', None)
    peers = mesh.shape['sp']

    def device_step(image_tokens, ln1_gain, ln1_shift, w_qkv, b_qkv, w_out, b_out, ln2_gain, ln2_shift, w_up, b_up, w_down, b_down):
        layers, width, _, heads, head_dim = w_qkv.shape
        mlp = w_up.shape[-1]
        images, share, _ = image_tokens.shape
        slots, tokens = images // peers, share * peers
        wq_t = jnp.transpose(w_qkv, (0, 2, 3, 4, 1)).reshape(layers, 3 * width, width)
        wu_t = jnp.transpose(w_up, (0, 2, 1))
        wo = w_out.reshape(layers, width, width)
        bq = b_qkv.reshape(layers, 3 * heads, head_dim)
        hbm = pl.BlockSpec(memory_space=pl.ANY)
        vmem = pl.BlockSpec(memory_space=pltpu.VMEM)
        dma = pltpu.SemaphoreType.DMA
        return pl.pallas_call(
            functools.partial(encoder_kernel, ('dp', 'sp'), heads, head_dim),
            out_shape=pltpu.VMEM(image_tokens.shape, image_tokens.dtype),
            in_specs=[hbm] * 13,
            out_specs=vmem,
            scratch_shapes=[
                pltpu.VMEM((slots, tokens, width), BF16),
                pltpu.VMEM(image_tokens.shape, BF16),
                pltpu.VMEM((3 * width, width), BF16),
                pltpu.VMEM((width, width), BF16),
                pltpu.VMEM((mlp, width), BF16),
                pltpu.VMEM((mlp, width), BF16),
                pltpu.VMEM(bq.shape, F32),
                pltpu.VMEM((layers, mlp), F32),
                *[pltpu.VMEM((layers, width), F32)] * 6,
                pltpu.VMEM((layers, 3 * width, LANES), F32),
                pltpu.VMEM((layers, mlp, LANES), F32),
                *[pltpu.VMEM((tokens, width), BF16)] * 4,
                pltpu.VMEM((3 * width, tokens), BF16),
                pltpu.VMEM((width, tokens), BF16),
                pltpu.VMEM((mlp, tokens), BF16),
                pltpu.VMEM((DEPTH, tokens, tokens), F32),
                pltpu.VMEM((DEPTH, tokens, tokens), BF16),
                dma((4,)), dma((8,)), dma((1,)), dma((slots, peers)), dma((slots, peers)), dma((slots,)),
                dma((slots, peers)), dma((slots, peers)), dma((slots,)),
            ],
            compiler_params=pltpu.CompilerParams(collective_id=0, has_side_effects=True, vmem_limit_bytes=60000 * 1024),
        )(image_tokens, wq_t, wo, wu_t, w_down, bq, b_up, ln1_gain, ln1_shift, b_out, ln2_gain, ln2_shift, b_down)

    return jax.shard_map(device_step, mesh=mesh, in_specs=(token_spec,) + (P(),) * 12, out_specs=token_spec, check_vma=False)
```
